32 devices in a mesh: views: 2 (over x), depth: 16 (over z, y, core).
Axes of the slice: x: 2, y: 2, z: 4, core: 2. Of those that a mesh axis runs over, the one named last changes fastest.
Arguments:
- density: float32 [512, 128, 256], P(('views', 'depth')), parts along dimension 0, may hold values from 0.2 to 5
- emission: bfloat16 [6, 256, 128, 256], P('views', 'depth'), parts along dimension 0, may hold values from 0 to 1
- occupancy: int32 [32, 4, 4], P(('views', 'depth')), parts along dimension 0, may hold values 0 or 1
- facing: int32 [2], P('views'), parts along dimension 0, may hold values from 0 to 1
Outputs:
- image: float32 [8, 128, 256], P('views', 'depth'), parts along dimension 0
The draws below stay inside these ranges and needn't reach their ends.
There are 2 independent parts, one for each index of `views`. The reference program is written for one: setup_inputs(seed, part) draws one part's arguments, and reference() takes and returns one part's arrays. A program takes and returns all parts, laid end to end along the dimension named above; each array names one. Nothing has to cross between parts.
Inputs may be any that keep to these rules, and one draw needn't show every extreme that they name: `occupancy`: 1 where the tile of the brick is occupied; where it is 0 the tile's cells neither absorb nor emit. `facing`: 0: bricks and cells of lower depth index are nearer the camera; 1: those of higher index.
All inputs are finite; a program needn't handle non-finite values. No bound on the sum of `occupancy` on one device may be relied on, other than what follows from the above.
Results may differ from the reference program's by a relative error of at most 0.0003.
Values sent between devices are 32-bit elements; how exact they have to be, the bound alone decides.
A program may use at most 128 MiB of HBM per device.

```python
import math
import jax
import jax.numpy as jnp
from jax import lax

IMG_H = 128
IMG_W = 256
DEPTH_DEV = 16
BRICKS = 16
NZ = 256
TILES_H = 4
TILES_W = 4
N_DEPTH = 16


def plant(values, rng, smallest, top_value):
    longest = values.shape.index(max(values.shape))
    spots = []
    for shift in (0, 1):
        where = [jax.random.randint(jax.random.fold_in(rng, axis), (), 0, length) for axis, length in enumerate(values.shape)]
        where[longest] = (where[longest] + shift) % values.shape[longest]
        spots.append(tuple(where))
    return values.at[spots[0]].set(smallest).at[spots[1]].set(top_value)


def block_levels(stream_key, dims, shards, smallest, top_value):
    factor_of = 1.0
    for position, parts in shards:
        heights = jax.random.uniform(jax.random.fold_in(jax.random.fold_in(stream_key, 6), position), (parts,), jnp.float32, smallest / len(shards), top_value / len(shards))
        factor_of = factor_of * jnp.repeat(jnp.exp(heights), dims[position] // parts).reshape((-1,) + (1,) * (len(dims) - 1 - position))
    return factor_of


def setup_inputs(seed: int = 0, part: int = 0) -> dict:
    arg_keys = jax.random.split(jax.random.key(seed), 5)
    own_keys = jax.random.split(jax.random.fold_in(arg_keys[4], part), 5)
    density = jnp.clip(jnp.exp(math.log(5.0) - 3.218876 * jax.random.uniform(own_keys[0], (NZ, IMG_H, IMG_W), jnp.float32) ** block_levels(own_keys[0], (NZ, IMG_H, IMG_W), ((0, 16),), -0.2, 0.2)), 0.2, 5.0)
    emission = jnp.clip(1.0 * jax.random.uniform(own_keys[1], (3, NZ, IMG_H, IMG_W), jnp.float32) ** block_levels(own_keys[1], (3, NZ, IMG_H, IMG_W), ((1, 16),), -0.2, 0.2), 0.0, 1.0).astype(jnp.bfloat16)
    occupancy = plant((jax.random.randint(own_keys[2], (BRICKS, TILES_H, TILES_W), 0, 4) < 3).astype(jnp.int32), jax.random.fold_in(own_keys[2], 1), 0, 1)
    facing = jax.random.randint(own_keys[3], (1,), 0, 2).astype(jnp.int32)
    return dict(density=density, emission=emission, occupancy=occupancy, facing=facing)


def march(dense, emitted, occupied, facing, bricks):
    depth_len, height, width = dense.shape
    tiles_h, tiles_w = occupied.shape
    gating = occupied.astype(jnp.float32)[None, :, None, :, None]
    optical = (dense.reshape(depth_len, tiles_h, height // tiles_h, tiles_w, width // tiles_w) * gating).reshape(dense.shape) / (depth_len * bricks)
    column = jnp.cumsum(optical, axis=0)
    whole = column[-1]
    ahead = jnp.where(facing == 0, column - optical, whole[None] - column)
    weight = (1.0 - jnp.exp(-optical)) * jnp.exp(-ahead)
    radiance = jnp.sum(emitted.astype(jnp.float32) * weight[None], axis=1)
    return radiance, jnp.exp(-whole)


def composite(radiance, transmit, facing):
    ones_row = jnp.ones_like(transmit[:1])
    forward = jnp.cumprod(transmit, axis=0)
    ahead_forward = jnp.concatenate([ones_row, forward[:-1]], axis=0)
    backward = jnp.flip(jnp.cumprod(jnp.flip(transmit, 0), axis=0), 0)
    ahead_backward = jnp.concatenate([backward[1:], ones_row], axis=0)
    front = jnp.where(facing == 0, ahead_forward, ahead_backward)
    colour = jnp.sum(radiance * front, axis=0)
    opacity = 1.0 - forward[-1]
    return jnp.concatenate([colour, opacity], axis=0)


def reference(density, emission, occupancy, facing):
    def single(brick_index):
        dense = lax.dynamic_slice_in_dim(density, brick_index * DEPTH_DEV, DEPTH_DEV, 0)
        emitted = lax.dynamic_slice_in_dim(emission, brick_index * DEPTH_DEV, DEPTH_DEV, 1)
        occupied = lax.dynamic_index_in_dim(occupancy, brick_index, 0, keepdims=False)
        return march(dense, emitted, occupied, facing[0], N_DEPTH)

    radiance, transmit = lax.map(single, jnp.arange(N_DEPTH, dtype=jnp.int32))
    return composite(radiance, transmit[:, None], facing[0])
```

```python
import functools
import math

import jax
import jax.numpy as jnp
from jax import lax
from jax.experimental import pallas as pl
from jax.experimental.pallas import tpu as pltpu
from jax.sharding import PartitionSpec as P

MESH = pl.DeviceIdType.MESH
STEP_ROWS = 16


def over(mine, theirs, mine_near):
    keep = mine_near + (1.0 - mine_near) * theirs[3]
    gain = (1.0 - mine_near) + mine_near * mine[3]
    colour = mine[:3] * keep[None] + theirs[:3] * gain[None]
    return colour, mine[3] * theirs[3]


def kernel(
    n, occ_ref, facing_ref, dens_hbm, emis_hbm, out_ref,
    dens, emis, loc, got1, pair, got2, quad, got3,
    dens_sem, emis_sem, send1, recv1, send2, recv2, send3, recv3,
):
    groups = n // 4
    depth_len, height, width = dens_hbm.shape
    rows = height // groups
    tile = rows // 4
    tiles_h, tiles_w = occ_ref.shape[1:]
    tile_rows, tile_cols = height // tiles_h, width // tiles_w
    step = min(STEP_ROWS, rows)

    me = lax.axis_index("depth")
    core = lax.rem(me, 2)
    side = lax.rem(me // 2, 2)
    group = me // 4
    core_peer = group * 4 + side * 2 + (1 - core)
    side_peer = group * 4 + (1 - side) * 2 + core

    def target(k):
        if k == groups - 1:
            return group
        down = jnp.where(groups - 1 - k > group, groups - 1 - k, groups - 2 - k)
        up = jnp.where(k < group, k, k + 1)
        return jnp.where(group < groups // 2, down, up)

    targets = [target(k) for k in range(groups)]
    loads = []
    for k in range(groups):
        span = pl.ds(pl.multiple_of(targets[k] * rows, rows), rows)
        loads.append((
            pltpu.make_async_copy(dens_hbm.at[:, span, :], dens.at[k], dens_sem.at[k]),
            pltpu.make_async_copy(emis_hbm.at[:, :, span, :], emis.at[k], emis_sem.at[k]),
        ))
    for load in loads:
        load[0].start()
        load[1].start()

    barrier = pltpu.get_barrier_semaphore()
    peers = [core_peer, side_peer]
    for off in range(1, groups):
        peers.append(lax.rem(group + off, groups) * 4 + side * 2 + core)
    for peer in peers:
        pl.semaphore_signal(barrier, inc=1, device_id={"depth": peer}, device_id_type=MESH)

    flip = facing_ref[0].astype(jnp.float32)
    sign = 1.0 - 2.0 * flip
    base = -math.log2(math.e) / (depth_len * n)
    col_tile = lax.broadcasted_iota(jnp.int32, (1, width), 1) // tile_cols

    def march(k):
        loads[k][0].wait()
        loads[k][1].wait()
        for row0 in range(0, rows, step):
            tile_row = (targets[k] * rows + row0) // tile_rows
            gate = jnp.zeros((1, width), jnp.float32)
            for i in range(tiles_w):
                gate = jnp.where(col_tile == i, occ_ref[0, tile_row, i].astype(jnp.float32), gate)
            scale = jnp.broadcast_to(gate * base, (step, width))
            cells = [dens[k, z, row0:row0 + step, :] for z in range(depth_len)]
            total = cells[0]
            for z in range(1, depth_len):
                total = total + cells[z]
            total = total * scale
            level = total * flip
            signed = scale * sign
            glow = jnp.exp2(level)
            sums = [jnp.zeros((step, width), jnp.float32) for _ in range(3)]
            for z in range(depth_len):
                level = level + signed * cells[z]
                later = jnp.exp2(level)
                weight = glow - later
                glow = later
                for c in range(3):
                    sums[c] = sums[c] + emis[k, c, z, row0:row0 + step, :].astype(jnp.float32) * weight
            planes = [s * sign for s in sums] + [jnp.exp2(total)]
            for t in range(step // tile):
                spot = row0 // tile + t
                for c in range(4):
                    loc[k, spot % 2, spot // 2, c] = planes[c][t * tile:(t + 1) * tile]

    def copy1(k):
        return pltpu.make_async_remote_copy(
            src_ref=loc.at[k, 1 - core], dst_ref=got1.at[k],
            send_sem=send1.at[k], recv_sem=recv1.at[k],
            device_id={"depth": core_peer}, device_id_type=MESH)

    def copy2(k):
        return pltpu.make_async_remote_copy(
            src_ref=pair.at[k, 1 - side], dst_ref=got2.at[k],
            send_sem=send2.at[k], recv_sem=recv2.at[k],
            device_id={"depth": side_peer}, device_id_type=MESH)

    def copy3(k):
        return pltpu.make_async_remote_copy(
            src_ref=quad.at[k], dst_ref=got3.at[group],
            send_sem=send3.at[k], recv_sem=recv3.at[group],
            device_id={"depth": targets[k] * 4 + side * 2 + core}, device_id_type=MESH)

    core_near = 1.0 - jnp.abs(core.astype(jnp.float32) - flip)
    side_near = 1.0 - jnp.abs(side.astype(jnp.float32) - flip)

    def merge1(k):
        copy1(k).wait_recv()
        for s in range(2):
            colour, clear = over(loc[k, core, s], got1[k, s], core_near)
            pair[k, s, :3] = colour
            pair[k, s, 3] = clear
        copy2(k).start()

    def merge2(k):
        copy2(k).wait_recv()
        colour, clear = over(pair[k, side], got2[k], side_near)
        if k == groups - 1:
            got3[group, :3] = colour
            got3[group, 3] = clear
        else:
            quad[k, :3] = colour
            quad[k, 3] = clear
            copy3(k).start()

    for k in range(groups):
        march(k)
        if k == 0:
            pl.semaphore_wait(barrier, len(peers))
        copy1(k).start()
        if k >= 2:
            merge1(k - 2)
    for k in range(max(groups - 2, 0), groups):
        merge1(k)
    for k in range(groups):
        merge2(k)

    for off in range(1, groups):
        source = lax.rem(group + off, groups)
        pltpu.make_async_remote_copy(
            src_ref=quad.at[0], dst_ref=got3.at[source],
            send_sem=send3.at[0], recv_sem=recv3.at[source],
            device_id={"depth": core_peer}, device_id_type=MESH).wait_recv()
    colour, clear = got3[0, :3], got3[0, 3]
    for g in range(1, groups):
        more, more_clear = got3[g, :3], got3[g, 3]
        keep = (1.0 - flip) + flip * more_clear
        gain = flip + (1.0 - flip) * clear
        colour = colour * keep[None] + more * gain[None]
        clear = clear * more_clear
    out_ref[:3] = colour
    out_ref[3] = 1.0 - clear

    for k in range(groups):
        copy1(k).wait_send()
        copy2(k).wait_send()
        if k < groups - 1:
            copy3(k).wait_send()


def on_device(n, density, emission, occupancy, facing):
    depth_len, height, width = density.shape
    groups = n // 4
    rows = height // groups
    tile = rows // 4
    smem = pl.BlockSpec(memory_space=pltpu.SMEM)
    hbm = pl.BlockSpec(memory_space=pl.ANY)
    dma = pltpu.SemaphoreType.DMA((groups,))
    return pl.pallas_call(
        functools.partial(kernel, n),
        out_shape=jax.ShapeDtypeStruct((4, tile, width), jnp.float32),
        in_specs=[smem, smem, hbm, hbm],
        out_specs=pl.BlockSpec(memory_space=pltpu.VMEM),
        scratch_shapes=[
            pltpu.VMEM((groups, depth_len, rows, width), density.dtype),
            pltpu.VMEM((groups, 3, depth_len, rows, width), emission.dtype),
            pltpu.VMEM((groups, 2, 2, 4, tile, width), jnp.float32),
            pltpu.VMEM((groups, 2, 4, tile, width), jnp.float32),
            pltpu.VMEM((groups, 2, 4, tile, width), jnp.float32),
            pltpu.VMEM((groups, 4, tile, width), jnp.float32),
            pltpu.VMEM((groups, 4, tile, width), jnp.float32),
            pltpu.VMEM((groups, 4, tile, width), jnp.float32),
        ] + [dma] * 8,
        compiler_params=pltpu.CompilerParams(collective_id=0, has_side_effects=True),
        name="render",
    )(occupancy, facing, density, emission)


def solution(mesh):
    return jax.shard_map(
        functools.partial(on_device, mesh.shape["depth"]),
        mesh=mesh,
        in_specs=(
            P(("views", "depth"), None, None),
            P("views", "depth", None, None),
            P(("views", "depth"), None, None),
            P("views"),
        ),
        out_specs=P("views", "depth", None),
        check_vma=False,
    )
```
